32 devices in a mesh: shot: 8 (over z, y), grid: 4 (over x, core).
Axes of the slice: x: 2, y: 2, z: 4, core: 2. Of those that a mesh axis runs over, the one named last changes fastest.
Arguments:
- residuals: bfloat16 [2048, 4, 512], P('shot', None, 'grid'), may hold values from -6 to 6
- encoding: bfloat16 [8, 2048], P(None, 'shot'), may hold values from -0.1875 to 0.1875
- receiver_cells: int32 [3, 512], replicated, may hold values from 0 to 127, as said below
- velocity_term: float32 [64, 128, 256], P('grid'), may hold values from 0.02 to 0.18
- field_before: float32 [8, 64, 128, 256], P('shot', 'grid'), may hold values from -6 to 6
- field_start: float32 [8, 64, 128, 256], P('shot', 'grid'), may hold values from -6 to 6
Outputs:
- field_last: float32 [8, 64, 128, 256], P('shot', 'grid')
- field_end: float32 [8, 64, 128, 256], P('shot', 'grid')
The draws below stay inside these ranges and needn't reach their ends.
Inputs may be any that keep to these rules, and one draw needn't show every extreme that they name: `receiver_cells`: row 0 holds first-dimension cells below 64, row 1 second-dimension cells below 128, row 2 third-dimension cells below 8.
All inputs are finite; a program needn't handle non-finite values.
Results may differ from the reference program's by a relative error of at most 0.0003.
Values sent between devices are 32-bit elements; how exact they have to be, the bound alone decides.
No kernel may reach another device: no remote copies, remote signals or barrier semaphores. Data moves between devices by JAX's collectives and lax.ppermute only.
A program may use at most 128 MiB of HBM per device.

```python
import math
import jax
import jax.numpy as jnp
from jax import lax

NY = 128
NZ = 256
STEPS = 4
SUPERSHOTS = 8
SHOTS = 2048
RECEIVERS = 512
NX = 64


def draw_receiver_cells(key, part):
    first_key, second_key, third_key = jax.random.split(jax.random.fold_in(key, 17), 3)
    first = jax.random.randint(first_key, (RECEIVERS,), 0, NX)
    second = jax.random.randint(second_key, (RECEIVERS,), 0, NY)
    third = jax.random.randint(third_key, (RECEIVERS,), 0, 8)
    return jnp.stack([first, second, third]).astype(jnp.int32)


def spiked(result, stream_key, source, target, parts, factor):
    def block_of(dim):
        return (jnp.arange(result.shape[dim]) // (result.shape[dim] // parts)).reshape((-1,) + (1,) * (result.ndim - 1 - dim))

    first = jax.random.permutation(stream_key, parts)[block_of(target)]
    far = (block_of(target) + parts // 2) % parts
    return jnp.where((block_of(source) == first) | (block_of(source) == far), factor * result, result)


def block_levels(own_key, shape, shards, low, high):
    factor_of = 1.0
    for axis_at, blocks in shards:
        steps = jax.random.uniform(jax.random.fold_in(jax.random.fold_in(own_key, 6), axis_at), (blocks,), jnp.float32, low / len(shards), high / len(shards))
        factor_of = factor_of * jnp.repeat(jnp.exp(steps), shape[axis_at] // blocks).reshape((-1,) + (1,) * (len(shape) - 1 - axis_at))
    return factor_of


def bell_draw(rng, shape, scale, limit, cuts=(), held_as=jnp.bfloat16):
    values = scale * jax.random.normal(rng, shape, jnp.float32)
    if cuts:
        values = values * block_levels(rng, shape, cuts, -0.22, 0.18)
    return jnp.clip(values, -limit, limit).astype(held_as)


def bell_draw_with(stream_key, shape, spread, bound, pieces, heavy, dtype=jnp.bfloat16):
    entries = spread * jax.random.normal(stream_key, shape, jnp.float32)
    if pieces:
        entries = entries * block_levels(stream_key, shape, pieces, -0.22, 0.18)
    return jnp.clip(spiked(entries, jax.random.fold_in(stream_key, 3), *heavy), -bound, bound).astype(dtype)


def setup_inputs(seed: int = 0) -> dict:
    key_of = jax.random.split(jax.random.key(seed), 7)
    return {
        "residuals": bell_draw(key_of[0], (SHOTS, STEPS, RECEIVERS), 1.0, 6.0, ((0, 8), (2, 4))),
        "encoding": bell_draw_with(key_of[1], (SUPERSHOTS, SHOTS), SHOTS ** -0.5, 0.1875, ((1, 8),), (1, 0, 8, 2.0)),
        "receiver_cells": draw_receiver_cells(jax.random.fold_in(key_of[6], 71), 0),
        "velocity_term": jnp.clip(jnp.exp(math.log(0.18) - 2.1972246 * jax.random.uniform(key_of[3], (NX, NY, NZ), jnp.float32) ** block_levels(key_of[3], (NX, NY, NZ), ((0, 4),), -0.2, 0.2)), 0.02, 0.18),
        "field_before": bell_draw(key_of[4], (SUPERSHOTS, NX, NY, NZ), 1.0, 6.0, ((0, 8), (1, 4)), jnp.float32),
        "field_start": bell_draw(key_of[5], (SUPERSHOTS, NX, NY, NZ), 1.0, 6.0, ((0, 8), (1, 4)), jnp.float32),
    }


coeffs = (-205.0 / 72.0, 8.0 / 5.0, -1.0 / 5.0, 8.0 / 315.0, -1.0 / 560.0)


def laplace(extended):
    width = extended.shape[0] - 8
    center = extended[4:4 + width]
    padded = jnp.pad(center, ((0, 0), (4, 4), (4, 4)))
    rows = center.shape[1]
    depth = center.shape[2]
    total = 3.0 * coeffs[0] * center
    for shift in range(1, 5):
        along_x = extended[4 + shift:4 + shift + width] + extended[4 - shift:4 - shift + width]
        along_y = padded[:, 4 + shift:4 + shift + rows, 4:4 + depth] + padded[:, 4 - shift:4 - shift + rows, 4:4 + depth]
        along_z = padded[:, 4:4 + rows, 4 + shift:4 + shift + depth] + padded[:, 4:4 + rows, 4 - shift:4 - shift + depth]
        total = total + coeffs[shift] * (along_x + along_y + along_z)
    return total


def inject(field, start_x, cells, values):
    width, rows, depth = field.shape
    local_x = cells[0] - start_x
    inside = (local_x >= 0) & (local_x < width)
    flat = (local_x * rows + cells[1]) * depth + cells[2]
    flat = jnp.where(inside, flat, width * rows * depth).astype(jnp.int32)
    return field.reshape(-1).at[flat].add(values, mode="drop").reshape(field.shape)


def reference(residuals, encoding, receiver_cells, velocity_term, field_before, field_start):
    encoded = jnp.dot(encoding, residuals.reshape(SHOTS, STEPS * RECEIVERS), preferred_element_type=jnp.float32)
    encoded = encoded.reshape(SUPERSHOTS, STEPS, RECEIVERS)

    def propagate(items):
        previous, current, traces = items
        for step in range(STEPS):
            extended = jnp.pad(current, ((4, 4), (0, 0), (0, 0)))
            advanced = 2.0 * current - previous + velocity_term * laplace(extended)
            advanced = inject(advanced, 0, receiver_cells, traces[STEPS - 1 - step])
            previous, current = current, advanced
        return previous, current

    field_last, field_end = lax.map(propagate, (field_before, field_start, encoded))
    return field_last, field_end
```

```python
import functools

import jax
import jax.numpy as jnp
import numpy as np
from jax import lax
from jax.experimental import pallas as pl
from jax.experimental.pallas import tpu as pltpu
from jax.sharding import PartitionSpec as P

scale = 5040.0
weights = (-14350.0, 8064.0, -1008.0, 128.0, -9.0)
coeffs = tuple(w / scale for w in weights)
reach = 4
near = 8
lanes = 128

VMEM = pl.BlockSpec(memory_space=pltpu.VMEM)
HBM = pl.BlockSpec(memory_space=pltpu.HBM)


def band(size):
    offset = np.abs(np.arange(size)[:, None] - np.arange(size)[None, :])
    table = np.zeros((size, size), np.float32)
    for j in range(1, reach + 1):
        table[offset == j] = weights[j]
    return table


def odd_device():
    return lax.rem(lax.axis_index("grid"), 2)


def pick(odd, if_odd, if_even):
    return odd * if_odd + (1 - odd) * if_even


def part_of(parts, u):
    first, middle, last = parts
    if u < reach:
        return first.at[u]
    if u < reach + middle.shape[0]:
        return middle.at[u - reach]
    return last.at[u - reach - middle.shape[0]]


def raw_of(ref, odd, u):
    width = ref.shape[-3]
    at = pick(odd, u, width - 1 - u)
    return ref.at[0, at] if len(ref.shape) == 4 else ref.at[at]


def step_kernel(raw_cur, raw_prev, injected, final, width, *refs):
    refs = list(refs)
    take = lambda n: tuple(refs.pop(0) for _ in range(n))
    cur_parts = take(1 if raw_cur else 3)
    prev_parts = take(1 if raw_prev else 3) if not (raw_cur and False) else ()
    (vel, halo, zband, yband) = take(4)
    inject = take(1)[0] if injected else None
    outs = take(2 if final else 3)
    sums = take(1)[0]
    odd = odd_device()
    rows, depth = vel.shape[1], vel.shape[2]

    def cur(u):
        if u < 0:
            k = -1 - u
            return halo.at[pick(odd, reach - 1 - k, k)] if raw_cur else halo.at[k]
        return raw_of(cur_parts[0], odd, u) if raw_cur else part_of(cur_parts, u)

    def prev(u):
        return raw_of(prev_parts[0], odd, u) if raw_prev else part_of(prev_parts, u)

    if final:
        whole, last = outs
        ready, sem = take(2)

        def out(u):
            return ready.at[u] if u < width - reach else last.at[u - width + reach]

        def copy(u):
            return pltpu.make_async_copy(ready.at[u], raw_of(whole, odd, u), sem.at[u])
    else:

        def out(u):
            return part_of(outs, u)

    chunk = 32
    for u in range(width):
        field = cur(u)[...]
        high = field.astype(jnp.bfloat16)
        low = (field - high.astype(jnp.float32)).astype(jnp.bfloat16)
        along_z = jnp.dot(jnp.concatenate([high, low], axis=1), zband[...], preferred_element_type=jnp.float32)
        along_y = jnp.dot(yband[...], jnp.concatenate([high, low], axis=0), preferred_element_type=jnp.float32)
        sums[u] = along_y + along_z
        for at in range(0, rows, chunk):
            part = pl.ds(at, min(chunk, rows - at))
            here = cur(u)[part, :]
            total = sums[u, part, :] * (1.0 / scale) + (3.0 * coeffs[0]) * here
            for j in range(1, reach + 1):
                pair = cur(u - j)[part, :]
                if u + j < width:
                    pair = pair + cur(u + j)[part, :]
                total = total + coeffs[j] * pair
            result = (here + here) - prev(u)[part, :] + raw_of(vel, odd, u)[part, :] * total
            out(u)[part, :] = result
            if injected:
                out(u)[part, :lanes] = result[:, :lanes] + inject[u, part, :]
        if final and 1 <= u <= width - reach:
            copy(u - 1).start()
    if final:
        for u in range(width - reach):
            copy(u).wait()


def edge_kernel(raw, injected, final, width, *refs):
    refs = list(refs)
    take = lambda n: tuple(refs.pop(0) for _ in range(n))
    (partial, vel, halo) = take(3)
    inject = take(1)[0] if injected else None
    if final:
        take(1)
    out = take(1)[0]
    if final:
        result, sem = take(2)
    else:
        result = out
    odd = odd_device()
    rows = vel.shape[1]
    chunk = 32

    def copy(i):
        return pltpu.make_async_copy(result.at[i], raw_of(out, odd, width - reach + i), sem.at[i])

    for i in range(reach):
        u = width - reach + i
        for at in range(0, rows, chunk):
            part = pl.ds(at, min(chunk, rows - at))
            total = None
            small = None
            for j in range(reach - i, reach + 1):
                h = i + j - reach
                index = pick(odd, h, reach - 1 - h) if raw else reach - 1 - h
                term = coeffs[j] * halo[index, part, :]
                total = term if total is None else total + term
                if injected:
                    term = coeffs[j] * inject[reach - 1 - h, part, :]
                    small = term if small is None else small + term
            factor = raw_of(vel, odd, u)[part, :]
            value = partial[i, part, :] + factor * total
            result[i, part, :] = value
            if injected:
                result[i, part, :lanes] = value[:, :lanes] + factor[:, :lanes] * small
        if final and i >= 1:
            copy(i - 1).start()
    if final:
        copy(reach - 1).start()
        for i in range(reach):
            copy(i).wait()


def inject_kernel(shots, samples, width, sent, cells, first, middle, last, halo, o_first, o_middle, o_last, o_halo, o_edge, *o_steps):
    odd = odd_device()
    groups = sent.shape[0] // shots
    own = sent.shape[1] // samples
    rows = first.shape[1]
    start = lax.axis_index("grid") * width
    traces = sent[0:groups, :]
    for s in range(1, shots):
        traces = traces + sent[s * groups : (s + 1) * groups, :]
    margin = lanes // near
    totals = [None] * samples
    per = max(1, 512 // own)
    for g0 in range(0, groups, per):
        gs = range(g0, min(groups, g0 + per))
        span = slice(g0 * own, (gs[-1] + 1) * own)
        x = cells[0:1, span] - start
        u = pick(odd, x, width - 1 - x)
        y = cells[1:2, span]
        z = cells[2:3, span]
        count = y.shape[1]
        at_row = jnp.where(lax.broadcasted_iota(jnp.int32, (rows, count), 0) == y, 1.0, 0.0).astype(jnp.bfloat16)
        at_row = jnp.concatenate([at_row, at_row], axis=1)
        for n in range(samples):
            t = samples - 1 - n
            value = jnp.concatenate([traces[g : g + 1, t * own : (t + 1) * own] for g in gs], axis=1)
            size = (width + 2 * reach) * near if n == 0 else width * near
            low_u = -reach if n == 0 else 0
            inside = (u >= low_u) & (u < low_u + size // near)
            cell = jnp.where(inside, (u - low_u) * near + z, -1)
            weighted = jnp.where(lax.broadcasted_iota(jnp.int32, (size, count), 0) == cell, value, 0.0)
            high = weighted.astype(jnp.bfloat16)
            rest = weighted - high.astype(jnp.float32)
            mid = rest.astype(jnp.bfloat16)
            both = jnp.concatenate([high, mid], axis=1)
            out = lax.dot_general(at_row, both, (((1,), (1,)), ((), ())), preferred_element_type=jnp.float32)
            totals[n] = out if totals[n] is None else totals[n] + out
    inside = lax.broadcasted_iota(jnp.int32, (rows, lanes), 1) < near

    def spread(n, k):
        base = k * near // lanes * lanes
        tile = totals[n][:, base : base + lanes]
        if tile.shape[1] < lanes:
            tile = jnp.concatenate([tile, jnp.zeros((rows, lanes - tile.shape[1]), jnp.float32)], axis=1)
        shift = k * near - base
        moved = pltpu.roll(tile, lanes - shift, 1) if shift else tile
        return jnp.where(inside, moved, 0.0)

    for k in range(width + 2 * reach):
        u = k - reach
        extra = spread(0, k)
        if u >= width:
            o_edge[width + reach - 1 - u] = extra
            continue
        if u < 0:
            source, target = halo.at[-1 - u], o_halo.at[-1 - u]
        else:
            source = part_of((first, middle, last), u)
            target = part_of((o_first, o_middle, o_last), u)
        target[:, lanes:] = source[:, lanes:]
        target[:, :lanes] = source[:, :lanes] + extra
    for n in range(1, samples):
        for u in range(width):
            o_steps[n - 1][u] = spread(n, u)


def gather_kernel(width, first, middle, last, whole, sem):
    odd = odd_device()
    copies = [pltpu.make_async_copy(part_of((first, middle, last), u), raw_of(whole, odd, u), sem.at[u]) for u in range(width)]
    for copy in copies:
        copy.start()
    for copy in copies:
        copy.wait()


def params(mib):
    return pltpu.CompilerParams(vmem_limit_bytes=mib * 1024 * 1024)


def local(residuals, encoding, receiver_cells, velocity_term, field_before, field_start):
    shot_rows, samples, own = residuals.shape
    width, rows, depth = velocity_term.shape
    groups, shots = lax.axis_size("grid"), lax.axis_size("shot")
    odd = lax.axis_index("grid") % 2
    f32 = jnp.float32
    shape = lambda *s: jax.ShapeDtypeStruct(s, f32)
    core_pairs = [(i, i ^ 1) for i in range(groups) if i ^ 1 < groups]
    chip_pairs = [(i, j) for i in range(groups) for j in [((i + 1) ^ 1) - 1] if 0 <= j < groups]

    zband = jnp.asarray(np.concatenate([band(depth)] * 2, axis=0), jnp.bfloat16)
    yband = jnp.asarray(np.concatenate([band(rows)] * 2, axis=1), jnp.bfloat16)

    to_chip = lax.dynamic_slice_in_dim(field_start[0], odd * (width - reach), reach, 0)
    to_core = lax.dynamic_slice_in_dim(field_start[0], (1 - odd) * (width - reach), reach, 0)
    chip_halo = lax.ppermute(to_chip, "grid", chip_pairs)
    core_halo = lax.ppermute(to_core, "grid", core_pairs)

    partial = jnp.dot(encoding, residuals.reshape(shot_rows, samples * own), preferred_element_type=f32)
    sent = jnp.broadcast_to(partial[:, None], (shots, groups, samples * own)).reshape(shots * groups, samples * own)
    sent = lax.all_to_all(sent, ("shot", "grid"), 0, 0, tiled=True)

    middle = width - 2 * reach
    previous, current = (field_before,), (field_start,)
    injections = [None] * samples
    edge_injection = None
    for n in range(samples):
        final = n == samples - 1
        raw_cur, raw_prev = len(current) == 1, len(previous) == 1
        inject = injections[n]
        layer_parts = [shape(reach, rows, depth), shape(middle, rows, depth), shape(reach, rows, depth)]
        results = pl.pallas_call(
            functools.partial(step_kernel, raw_cur, raw_prev, inject is not None, final, width),
            out_shape=[shape(1, width, rows, depth), layer_parts[2]] if final else layer_parts,
            in_specs=[VMEM] * (len(current) + len(previous) + 4 + (inject is not None)),
            out_specs=[HBM, VMEM] if final else [VMEM] * 3,
            scratch_shapes=[pltpu.VMEM((width, rows, depth), f32)]
            + ([pltpu.VMEM((width - reach, rows, depth), f32), pltpu.SemaphoreType.DMA((width - reach,))] if final else []),
            compiler_params=params(24),
            cost_estimate=pl.CostEstimate(flops=900_000_000, bytes_accessed=8_000_000, transcendentals=0),
            name=f"step{n}",
        )(*current, *previous, velocity_term, core_halo, zband, yband, *(() if inject is None else (inject,)))
        partial_edge = results[-1]
        extra = () if edge_injection is None else (edge_injection,)
        if final:
            (end,) = pl.pallas_call(
                functools.partial(edge_kernel, raw_cur, bool(extra), True, width),
                out_shape=[shape(1, width, rows, depth)],
                in_specs=[VMEM] * (3 + len(extra)) + [HBM],
                out_specs=[HBM],
                scratch_shapes=[pltpu.VMEM((reach, rows, depth), f32), pltpu.SemaphoreType.DMA((reach,))],
                input_output_aliases={3 + len(extra): 0},
                compiler_params=params(16),
                name=f"edge{n}",
            )(partial_edge, velocity_term, chip_halo, *extra, results[0])
            (last,) = pl.pallas_call(
                functools.partial(gather_kernel, width),
                out_shape=[shape(1, width, rows, depth)],
                in_specs=[VMEM] * 3,
                out_specs=[HBM],
                scratch_shapes=[pltpu.SemaphoreType.DMA((width,))],
                compiler_params=params(16),
                name="gather",
            )(*current)
            return last, end
        (edge,) = pl.pallas_call(
            functools.partial(edge_kernel, raw_cur, bool(extra), False, width),
            out_shape=[layer_parts[2]],
            in_specs=[VMEM] * (3 + len(extra)),
            out_specs=[VMEM],
            compiler_params=params(16),
            cost_estimate=pl.CostEstimate(flops=100_000_000, bytes_accessed=2_000_000, transcendentals=0),
            name=f"edge{n}",
        )(partial_edge, velocity_term, chip_halo, *extra)
        chip_halo = lax.ppermute(edge, "grid", chip_pairs)
        core_halo = lax.ppermute(results[0], "grid", core_pairs)
        previous, current = current, (results[0], results[1], edge)
        edge_injection = None
        if n == 0:
            spread = pl.pallas_call(
                functools.partial(inject_kernel, shots, samples, width),
                out_shape=[*layer_parts, layer_parts[0], shape(reach, rows, lanes)] + [shape(width, rows, lanes)] * (samples - 1),
                in_specs=[VMEM] * 6,
                out_specs=[VMEM] * (4 + samples),
                compiler_params=params(24),
                cost_estimate=pl.CostEstimate(flops=400_000_000, bytes_accessed=8_000_000, transcendentals=0),
                name="inject",
            )(sent, receiver_cells, *current, core_halo)
            current = tuple(spread[:3])
            core_halo, edge_injection = spread[3], spread[4]
            injections[1:] = spread[5:]


def solution(mesh):
    return jax.shard_map(
        local,
        mesh=mesh,
        in_specs=(
            P("shot", None, "grid"),
            P(None, "shot"),
            P(),
            P("grid", None, None),
            P("shot", "grid", None, None),
            P("shot", "grid", None, None),
        ),
        out_specs=(P("shot", "grid", None, None), P("shot", "grid", None, None)),
        check_vma=False,
    )
```

```python
import functools

import jax
import jax.numpy as jnp
from jax import lax
from jax.experimental import pallas as pl
from jax.experimental.pallas import tpu as pltpu
from jax.sharding import PartitionSpec as P

scale = 5040.0
weights = (-14350.0, 8064.0, -1008.0, 128.0, -9.0)
coeffs = tuple(w / scale for w in weights)
reach = 4
near = 8
lanes = 128
chunk = 32
f32 = jnp.float32
bf16 = jnp.bfloat16

VMEM = pl.BlockSpec(memory_space=pltpu.VMEM)
HBM = pl.BlockSpec(memory_space=pltpu.HBM)


def odd_device():
    return lax.rem(lax.axis_index("grid"), 2)


def place(u, width):
    odd = odd_device()
    return odd * u + (1 - odd) * (width - 1 - u)


def raw_of(ref, u):
    at = place(u, ref.shape[-3])
    return ref.at[0, at] if len(ref.shape) == 4 else ref.at[at]


def slice_of(ref, u, mine, low=0):
    flip = odd_device() if mine else 1 - odd_device()
    return ref.at[low + flip * u + (1 - flip) * (reach - 1 - u)]


def part_of(parts, u):
    first, middle, last = parts
    if u < reach:
        return first.at[u]
    if u < reach + middle.shape[0]:
        return middle.at[u - reach]
    return last.at[u - reach - middle.shape[0]]


def band(size):
    offset = jnp.abs(lax.broadcasted_iota(jnp.int32, (size, size), 0) - lax.broadcasted_iota(jnp.int32, (size, size), 1))
    table = jnp.zeros((size, size), f32)
    for j in range(1, reach + 1):
        table = jnp.where(offset == j, weights[j], table)
    return table.astype(bf16)


def chunks(rows):
    return [pl.ds(at, min(chunk, rows - at)) for at in range(0, rows, chunk)]


def step_kernel(kind, width, *refs):
    refs = list(refs)
    take = lambda n: tuple(refs.pop(0) for _ in range(n))
    cur_parts = take(1 if kind == "start" else 3)
    prev_parts = take(1 if kind in ("start", "full") else 3)
    velocity, core_halo = take(2)
    inject = None if kind == "start" else take(1)[0]
    chip_halo = take(1)[0] if kind == "full" else None
    outs = take(2 if kind == "final" else 3)
    sums, zband, yband = take(3)
    rows, depth = velocity.shape[1], velocity.shape[2]

    def cur(u):
        if u < 0:
            return slice_of(core_halo, -1 - u, False) if kind == "start" else core_halo.at[-1 - u]
        if u >= width:
            return chip_halo.at[reach - 1 - (u - width)]
        return raw_of(cur_parts[0], u) if kind == "start" else part_of(cur_parts, u)

    def prev(u):
        return raw_of(prev_parts[0], u) if kind in ("start", "full") else part_of(prev_parts, u)

    if kind == "final":
        whole, last = outs
        ready, sem = take(2)

        def out(u):
            return ready.at[u] if u < width - reach else last.at[u - width + reach]

        def copy(u):
            return pltpu.make_async_copy(ready.at[u], raw_of(whole, u), sem.at[u])
    else:

        def out(u):
            return part_of(outs, u)

    along = band(depth)
    zband[:depth, :] = along
    zband[depth:, :] = along
    across = band(rows)
    yband[:, :rows] = across
    yband[:, rows:] = across
    for u in range(width):
        field = cur(u)[...]
        high = field.astype(bf16)
        low = (field - high.astype(f32)).astype(bf16)
        along_z = jnp.dot(jnp.concatenate([high, low], axis=1), zband[...], preferred_element_type=f32)
        along_y = jnp.dot(yband[...], jnp.concatenate([high, low], axis=0), preferred_element_type=f32)
        sums[u] = along_y + along_z
        for part in chunks(rows):
            here = cur(u)[part, :]
            total = sums[u, part, :] * (1.0 / scale) + (3.0 * coeffs[0]) * here
            for j in range(1, reach + 1):
                pair = cur(u - j)[part, :]
                if u + j < width or chip_halo is not None:
                    pair = pair + cur(u + j)[part, :]
                total = total + coeffs[j] * pair
            result = (here + here) - prev(u)[part, :] + raw_of(velocity, u)[part, :] * total
            out(u)[part, :] = result
            if inject is not None:
                out(u)[part, :lanes] = result[:, :lanes] + inject[u, part, :]
        if kind == "final" and 1 <= u <= width - reach:
            copy(u - 1).start()
    if kind == "final":
        for u in range(width - reach):
            copy(u).wait()


def edge_value(partial, factor, halo, i, part):
    total = None
    for j in range(reach - i, reach + 1):
        term = coeffs[j] * halo(reach - 1 - (i + j - reach))[part, :]
        total = term if total is None else total + term
    return partial[part, :] + factor[part, :] * total


def edge_kernel(width, partial, velocity, halo, out):
    for i in range(reach):
        for part in chunks(velocity.shape[1]):
            out[i, part, :] = edge_value(partial.at[i], raw_of(velocity, width - reach + i), lambda k: halo.at[k], i, part)


def last_edge_kernel(width, partial, velocity, halo_partial, halo_velocity, own, whole_in, whole, halo, result, sem):
    def copy(i):
        return pltpu.make_async_copy(result.at[i], raw_of(whole, width - reach + i), sem.at[i])

    parts = chunks(velocity.shape[1])
    for i in range(reach):
        for part in parts:
            halo[i, part, :] = edge_value(halo_partial.at[i], slice_of(halo_velocity, i, False, reach), lambda k: own.at[k], i, part)
    for i in range(reach):
        for part in parts:
            result[i, part, :] = edge_value(partial.at[i], raw_of(velocity, width - reach + i), lambda k: halo.at[k], i, part)
        if i >= 1:
            copy(i - 1).start()
    copy(reach - 1).start()
    for i in range(reach):
        copy(i).wait()


def fan_kernel(groups, partial, out):
    for k in range(partial.shape[0]):
        for g in range(groups):
            out[k * groups + g] = partial[k : k + 1, :]


def spread_traces(steps, shots, samples, width, rows, sent, cells):
    groups = sent.shape[0] // shots
    own = sent.shape[2] // samples
    start = lax.axis_index("grid") * width
    traces = []
    for g in range(groups):
        row = sent[g]
        for s in range(1, shots):
            row = row + sent[s * groups + g]
        traces.append(row)
    totals = {}
    per = max(1, 512 // own)
    for g0 in range(0, groups, per):
        gs = range(g0, min(groups, g0 + per))
        span = slice(g0 * own, (gs[-1] + 1) * own)
        u = place(cells[0:1, span] - start, width)
        y, z = cells[1:2, span], cells[2:3, span]
        count = y.shape[1]
        at_row = jnp.where(lax.broadcasted_iota(jnp.int32, (rows, count), 0) == y, 1.0, 0.0).astype(bf16)
        at_row = jnp.concatenate([at_row, at_row], axis=1)
        for n in steps:
            t = samples - 1 - n
            value = jnp.concatenate([traces[g][:, t * own : (t + 1) * own] for g in gs], axis=1)
            low_u = -reach if n == 0 else 0
            size = (width - 2 * low_u) * near
            inside = (u >= low_u) & (u < width - low_u)
            cell = jnp.where(inside, (u - low_u) * near + z, -1)
            weighted = jnp.where(lax.broadcasted_iota(jnp.int32, (size, count), 0) == cell, value, 0.0)
            high = weighted.astype(bf16)
            rest = (weighted - high.astype(f32)).astype(bf16)
            both = jnp.concatenate([high, rest], axis=1)
            out = lax.dot_general(at_row, both, (((1,), (1,)), ((), ())), preferred_element_type=f32)
            totals[n] = totals[n] + out if n in totals else out
    inside = lax.broadcasted_iota(jnp.int32, (rows, lanes), 1) < near

    def layer(n, u):
        at = (u + (reach if n == 0 else 0)) * near
        base = at // lanes * lanes
        tile = totals[n][:, base : base + lanes]
        if tile.shape[1] < lanes:
            tile = jnp.concatenate([tile, jnp.zeros((rows, lanes - tile.shape[1]), f32)], axis=1)
        moved = pltpu.roll(tile, lanes - (at - base), 1) if at > base else tile
        return jnp.where(inside, moved, 0.0)

    return layer


def inject_kernel(shots, samples, width, sent, cells, first, middle, partial, core_halo, velocity, chip_in, chip_partial, chip_own, *outs):
    o_first, o_middle, o_last, o_core, o_chip, o_step = outs
    rows = first.shape[1]
    layer = spread_traces((0, 1), shots, samples, width, rows, sent, cells)
    for i in range(reach):
        for part in chunks(rows):
            o_last[i, part, :] = edge_value(partial.at[i], raw_of(velocity, width - reach + i), lambda k: slice_of(chip_in, k, False), i, part)
            o_chip[i, part, :] = edge_value(chip_partial.at[i], slice_of(chip_in, i, False, reach), lambda k: slice_of(chip_own, k, True), i, part)
    for u in range(-reach, width + reach):
        extra = layer(0, u)
        if u >= width - reach:
            target = o_chip.at[reach - 1 - (u - width)] if u >= width else o_last.at[u - width + reach]
            target[:, :lanes] = target[:, :lanes] + extra
            continue
        if u < 0:
            source, target = core_halo.at[-1 - u], o_core.at[-1 - u]
        else:
            source, target = part_of((first, middle, None), u), part_of((o_first, o_middle, None), u)
        target[:, lanes:] = source[:, lanes:]
        target[:, :lanes] = source[:, :lanes] + extra
    for u in range(width):
        o_step[u] = layer(1, u)


def spread_kernel(steps, shots, samples, width, sent, cells, *outs):
    layer = spread_traces(steps, shots, samples, width, outs[0].shape[1], sent, cells)
    for n, out in zip(steps, outs):
        for u in range(width):
            out[u] = layer(n, u)


def gather_kernel(width, first, middle, last, whole, sem):
    copies = [pltpu.make_async_copy(part_of((first, middle, last), u), raw_of(whole, u), sem.at[u]) for u in range(width)]
    for copy in copies:
        copy.start()
    for copy in copies:
        copy.wait()


def call(kernel, name, ins, outs, scratch=(), in_hbm=(), out_hbm=(), mib=16, flops=100_000_000, aliases={}):
    return pl.pallas_call(
        kernel,
        out_shape=outs,
        in_specs=[HBM if k in in_hbm else VMEM for k in range(len(ins))],
        out_specs=[HBM if k in out_hbm else VMEM for k in range(len(outs))],
        scratch_shapes=list(scratch),
        input_output_aliases=aliases,
        compiler_params=pltpu.CompilerParams(vmem_limit_bytes=mib * 1024 * 1024),
        cost_estimate=pl.CostEstimate(flops=flops, bytes_accessed=1_000_000, transcendentals=0),
        name=name,
    )(*ins)


def local(residuals, encoding, receiver_cells, velocity, field_before, field_start):
    shot_rows, samples, own = residuals.shape
    width, rows, depth = velocity.shape
    groups, shots = lax.axis_size("grid"), lax.axis_size("shot")
    assert samples == 4 and width >= 2 * reach
    shape = lambda *s: jax.ShapeDtypeStruct(s, f32)
    four, whole, small = shape(reach, rows, depth), shape(1, width, rows, depth), shape(width, rows, lanes)
    parts = [four, shape(width - 2 * reach, rows, depth), four]
    core_pairs = [(i, i ^ 1) for i in range(groups) if i ^ 1 < groups]
    chip_pairs = [(i, j) for i in range(groups) for j in [((i + 1) ^ 1) - 1] if 0 <= j < groups]
    to_core = lambda x: lax.ppermute(x, "grid", core_pairs)
    to_chip = lambda x: lax.ppermute(x, "grid", chip_pairs)
    sums = pltpu.VMEM((width, rows, depth), f32)
    bands = [pltpu.VMEM((2 * depth, depth), bf16), pltpu.VMEM((rows, 2 * rows), bf16)]
    dma = pltpu.SemaphoreType.DMA
    step = lambda kind: functools.partial(step_kernel, kind, width)
    work = 900_000_000

    odd = odd_device()
    toward_chip = lambda x: lax.dynamic_slice_in_dim(x, odd * (width - reach), reach, 0)
    core_own = lax.dynamic_slice_in_dim(field_start[0], (1 - odd) * (width - reach), reach, 0)
    chip_own = jnp.concatenate([toward_chip(field_start[0]), toward_chip(velocity)], axis=0)
    core_halo = to_core(core_own)
    chip_in = to_chip(chip_own)
    first, middle, partial = call(
        step("start"), "step0", (field_start, field_before, velocity, core_halo), parts,
        [sums, *bands], flops=work,
    )
    core_halo = to_core(first)
    chip_partial = to_chip(partial)

    summed = jnp.dot(encoding, residuals.reshape(shot_rows, samples * own), preferred_element_type=f32)
    summed, _ = lax.optimization_barrier((summed, partial))
    (sent,) = call(functools.partial(fan_kernel, groups), "fan", (summed,), [shape(shots * groups, 1, samples * own)], mib=4)
    sent = lax.all_to_all(sent, ("shot", "grid"), 0, 0, tiled=True)

    *before, core_halo, chip_halo, source = call(
        functools.partial(inject_kernel, shots, samples, width), "inject",
        (sent, receiver_cells, first, middle, partial, core_halo, velocity, chip_in, chip_partial, chip_own),
        [*parts, four, four, small], flops=work,
    )
    current = call(
        step("full"), "step1", (*before, field_start, velocity, core_halo, source, chip_halo), parts, [sums, *bands], flops=work
    )
    core_halo = to_core(current[0])
    chip_halo = to_chip(current[2])
    sent, core_halo = lax.optimization_barrier((sent, core_halo))
    sources = call(
        functools.partial(spread_kernel, (2, 3), shots, samples, width), "spread", (sent, receiver_cells), [small, small], flops=work // 2
    )
    first, middle, partial = call(
        step("part"), "step2", (*current, *before, velocity, core_halo, sources[0]), parts, [sums, *bands], flops=work
    )
    core_halo = to_core(first)
    chip_partial = to_chip(partial)
    (last,) = call(functools.partial(edge_kernel, width), "edge", (partial, velocity, chip_halo), [four])
    end, partial = call(
        step("final"), "step3", (first, middle, last, *current, velocity, core_halo, sources[1]), [whole, four],
        [sums, *bands, pltpu.VMEM((width - reach, rows, depth), f32), dma((width - reach,))], out_hbm=(0,), flops=work,
    )
    (stored,) = call(functools.partial(gather_kernel, width), "gather", (first, middle, last), [whole], [dma((width,))], out_hbm=(0,))
    (end,) = call(
        functools.partial(last_edge_kernel, width), "last_edge", (partial, velocity, chip_partial, chip_in, current[2], end), [whole],
        [pltpu.VMEM((reach, rows, depth), f32), pltpu.VMEM((reach, rows, depth), f32), dma((reach,))], (5,), (0,), aliases={5: 0},
    )
    return stored, end


def solution(mesh):
    return jax.shard_map(
        local,
        mesh=mesh,
        in_specs=(
            P("shot", None, "grid"),
            P(None, "shot"),
            P(),
            P("grid", None, None),
            P("shot", "grid", None, None),
            P("shot", "grid", None, None),
        ),
        out_specs=(P("shot", "grid", None, None), P("shot", "grid", None, None)),
        check_vma=False,
    )
```
